32 devices in a mesh: gy: 16 (over z, y, core), gz: 2 (over x).
Axes of the slice: x: 2, y: 2, z: 4, core: 2. Of those that a mesh axis runs over, the one named last changes fastest.
Arguments:
- omega: float32 [3, 256, 128, 128], P(None, 'gy', 'gz'), may hold values from -6 to 6
- velocity: float32 [3, 256, 128, 128], P(None, 'gy', 'gz'), may hold values from -6 to 6
- point_owner: int32 [1152], replicated, may hold values from 0 to 22, as said below
- point_cells: int32 [3, 1152], replicated, may hold values from 1 to 125, as said below
- point_frac: float32 [3, 1152], replicated, may hold values from 0 to 1
- chord: float32 [1152], replicated, may hold values from 0.2 to 1
- twist: float32 [1152], replicated, may hold values from -0.3 to 0.3
- angle_step: int32 [1], replicated, may hold values from 0 to 719
Outputs:
- omega_out: float32 [3, 256, 128, 128], P(None, 'gy', 'gz')
- blade_sources: float32 [3, 1152], replicated
The draws below stay inside these ranges and needn't reach their ends.
Inputs may be any that keep to these rules, and one draw needn't show every extreme that they name: `point_owner`: turbine t's points lie in spanwise blocks t * 2 to (t + 1) * 2 - 1 and in the 1 vertical blocks from (1) // 2 on; no block holds more than 192 points, and in every turbine one block holds exactly 192. `point_cells`: streamwise cells lie in 1 to 125, spanwise in 1 to 13, vertical in 1 to 61; all points of a turbine share one streamwise cell.
All inputs are finite; a program needn't handle non-finite values.
Results may differ from the reference program's by a relative error of at most 0.0003.
Values sent between devices are 32-bit elements; how exact they have to be, the bound alone decides.
A program may use at most 128 MiB of HBM per device.

```python
import math
import jax
import jax.numpy as jnp
from jax import lax

CY = 16
CZ = 64
NX = 128
TURBINES = 6
BLADES = 3
BP = 64
NY = 256
NZ = 128
POINTS = 1152
MOST = 192
N_GZ = 2


def rotor_layout(key):
    span_count = NY // CY
    vert_count = NZ // CZ
    span_blocks = span_count // TURBINES
    vert_blocks = max(vert_count // 2, 1)
    blocks = span_blocks * vert_blocks
    slots = blocks * MOST
    per_rotor = BLADES * BP

    def one_rotor(rotor_key, rotor_number):
        chosen = jax.random.randint(jax.random.fold_in(rotor_key, 1), (), 0, blocks)
        packed = jnp.where(rotor_number == 0, 0, jnp.where(rotor_number == TURBINES - 1, blocks - 1, chosen))
        shuffle = jax.random.permutation(jax.random.fold_in(rotor_key, 2), slots).astype(jnp.int32)
        slot_block = jnp.arange(slots, dtype=jnp.int32) // MOST
        ranking = shuffle - slots * (slot_block == packed).astype(jnp.int32)
        order = jnp.argsort(ranking, stable=True)[:per_rotor]
        return (order // MOST).astype(jnp.int32)
    rotor_keys = jax.random.split(jax.random.fold_in(key, 77), TURBINES)
    rotor_numbers = jnp.arange(TURBINES, dtype=jnp.int32)
    block = jax.vmap(one_rotor)(rotor_keys, rotor_numbers)
    rotor = rotor_numbers[:, None]
    span_index = rotor * span_blocks + block // vert_blocks
    vert_index = (vert_count - vert_blocks) // 2 + block % vert_blocks
    owner = (span_index * vert_count + vert_index).reshape(-1).astype(jnp.int32)
    cell_key = jax.random.fold_in(key, 78)
    plane = jax.random.randint(jax.random.fold_in(cell_key, 1), (TURBINES, 1), 1, NX - 2)
    cell_x = jnp.broadcast_to(plane, (TURBINES, per_rotor)).reshape(-1)
    cell_y = jax.random.randint(jax.random.fold_in(cell_key, 2), (TURBINES * per_rotor,), 1, CY - 2)
    cell_z = jax.random.randint(jax.random.fold_in(cell_key, 3), (TURBINES * per_rotor,), 1, CZ - 2)
    cells = jnp.stack([cell_x, cell_y, cell_z]).astype(jnp.int32)
    return (owner, cells)


def draw_point_owner(key, part):
    return rotor_layout(key)[0]


def draw_point_cells(key, part):
    return rotor_layout(key)[1]


def shard_levels(rng, extent, pieces, low, high):
    def one(dim, blocks):
        steps = jax.random.uniform(jax.random.fold_in(jax.random.fold_in(rng, 6), dim), (blocks,), jnp.float32, low / len(pieces), high / len(pieces))
        return jnp.repeat(jnp.exp(steps), extent[dim] // blocks).reshape((-1,) + (1,) * (len(extent) - dim - 1))

    gain = one(*pieces[0])
    for cut in pieces[1:]:
        gain = gain * one(*cut)
    return gain


def scatter_about(rng, dims, deviation, limit, pieces=(), kind=jnp.bfloat16):
    factor_of = shard_levels(rng, dims, pieces, -0.22, 0.18) if pieces else 1.0
    values = jax.random.normal(rng, dims, jnp.float32) * deviation * factor_of
    return jnp.minimum(jnp.maximum(values, -limit), limit).astype(kind)


def setup_inputs(seed: int = 0) -> dict:
    splits = jax.random.split(jax.random.key(seed), 9)
    omega = scatter_about(splits[0], (3, NY, NZ, NX), 1.0, 6.0, ((1, 16), (2, 2)), jnp.float32)
    velocity = scatter_about(splits[1], (3, NY, NZ, NX), 1.0, 6.0, ((1, 16), (2, 2)), jnp.float32)
    point_owner = draw_point_owner(jax.random.fold_in(splits[8], 71), 0)
    point_cells = draw_point_cells(jax.random.fold_in(splits[8], 71), 0)
    point_frac = jnp.clip(jax.random.uniform(splits[4], (3, POINTS), jnp.float32, 0.0, 1.0), 0.0, 1.0)
    chord = jnp.clip(jnp.exp(jax.random.uniform(splits[5], (POINTS,), jnp.float32, math.log(0.2), math.log(1.0))), 0.2, 1.0)
    twist = jnp.clip(jax.random.uniform(splits[6], (POINTS,), jnp.float32, -0.3, 0.3), -0.3, 0.3)
    angle_step = jax.random.randint(splits[7], (1,), 0, 720).astype(jnp.int32)
    return dict(omega=omega, velocity=velocity, point_owner=point_owner, point_cells=point_cells, point_frac=point_frac, chord=chord, twist=twist, angle_step=angle_step)


section_step = 0.4
viscosity = 0.05
tip_speed = 3.0
turn_step = 2.0 * 3.141592653589793 / 720.0

def remesh_kernel(shift):
    mag = jnp.abs(shift)
    inner = 1.0 - 2.5 * mag * mag + 1.5 * mag * mag * mag
    outer = 0.5 * (2.0 - mag) * (2.0 - mag) * (1.0 - mag)
    return jnp.where(mag < 1.0, inner, jnp.where(mag < 2.0, outer, 0.0))

def shifted(padded, axis, offset):
    index = []
    for dim in range(4):
        if dim == 0:
            index.append(slice(None))
        elif dim == axis:
            index.append(slice(offset, offset + padded.shape[dim] - 4))
        else:
            index.append(slice(2, padded.shape[dim] - 2))
    return padded[tuple(index)]

def centered_first(padded, axis):
    return (shifted(padded, axis, 0) - 8.0 * shifted(padded, axis, 1) + 8.0 * shifted(padded, axis, 3) - shifted(padded, axis, 4)) / 12.0

def centered_second(padded, axis):
    return (-shifted(padded, axis, 0) + 16.0 * shifted(padded, axis, 1) - 30.0 * shifted(padded, axis, 2) + 16.0 * shifted(padded, axis, 3) - shifted(padded, axis, 4)) / 12.0

def remesh_padded(field, displace, axis):
    length = field.shape[axis] - 4
    total = jnp.zeros(field.shape[:axis] + (length,) + field.shape[axis + 1:], jnp.float32)
    for offset in range(-2, 3):
        start = 2 - offset
        part = lax.slice_in_dim(field, start, start + length, axis=axis)
        moved = lax.slice_in_dim(displace, start, start + length, axis=axis - 1)
        total = total + remesh_kernel(offset - moved)[None] * part
    return total

def blade_forces(point_velocity, chord, twist, angle_step):
    count = point_velocity.shape[1]
    points = jnp.arange(count, dtype=jnp.int32)
    station = points % BP
    blade = points // BP % BLADES
    theta = angle_step[0].astype(jnp.float32) * turn_step + 2.0 * 3.141592653589793 / 3.0 * blade.astype(jnp.float32)
    radius = (station.astype(jnp.float32) + 0.5) / BP
    cos_t = jnp.cos(theta)
    sin_t = jnp.sin(theta)
    rel_x = point_velocity[0]
    rel_y = point_velocity[1] + tip_speed * radius * sin_t
    rel_z = point_velocity[2] - tip_speed * radius * cos_t
    rel_t = -sin_t * rel_y + cos_t * rel_z
    speed = jnp.sqrt(rel_x * rel_x + rel_t * rel_t + 1.0)
    gamma = 3.141592653589793 * chord * (rel_x * jnp.cos(twist) + rel_t * jnp.sin(twist))
    blades = gamma.reshape(-1, BP)
    before = jnp.concatenate([jnp.zeros((blades.shape[0], 1), jnp.float32), blades[:, :-1]], axis=1)
    shed = (blades - before).reshape(-1)
    return jnp.stack([shed * rel_x / speed, gamma * cos_t + shed * rel_y / speed, gamma * sin_t + shed * rel_z / speed])

def reference(omega, velocity, point_owner, point_cells, point_frac, chord, twist, angle_step):
    owner_span = point_owner // N_GZ
    owner_vert = point_owner % N_GZ
    base_x = point_cells[0]
    base_y = owner_span * CY + point_cells[1]
    base_z = owner_vert * CZ + point_cells[2]
    steps = jnp.arange(-1, 3, dtype=jnp.int32)
    off_x = jnp.repeat(steps, 16)
    off_y = jnp.tile(jnp.repeat(steps, 4), 4)
    off_z = jnp.tile(steps, 16)
    index_x = (base_x[None, :] + off_x[:, None]).astype(jnp.int32)
    index_y = (base_y[None, :] + off_y[:, None]).astype(jnp.int32)
    index_z = (base_z[None, :] + off_z[:, None]).astype(jnp.int32)
    weight = remesh_kernel(off_x[:, None].astype(jnp.float32) - point_frac[0][None, :])
    weight = weight * remesh_kernel(off_y[:, None].astype(jnp.float32) - point_frac[1][None, :])
    weight = weight * remesh_kernel(off_z[:, None].astype(jnp.float32) - point_frac[2][None, :])
    sampled = velocity[:, index_y, index_z, index_x]
    point_velocity = lax.optimization_barrier(jnp.sum(sampled * weight[None], axis=1))
    sources = blade_forces(point_velocity, chord, twist, angle_step)
    smear = jnp.zeros_like(omega).at[:, index_y, index_z, index_x].add(sources[:, None, :] * weight[None])
    pads = ((0, 0), (2, 2), (2, 2), (2, 2))
    omega_pad = jnp.pad(omega, pads)
    velocity_pad = jnp.pad(velocity, pads)
    stretch = jnp.zeros_like(omega)
    laplace = jnp.zeros_like(omega)
    for axis in range(3):
        stretch = stretch + omega[2 - axis][None] * centered_first(velocity_pad, 3 - axis)
        laplace = laplace + centered_second(omega_pad, axis + 1)
    section = omega + section_step * (stretch + viscosity * laplace + smear)
    displace = jnp.clip(section_step * velocity, -1.0, 1.0)
    moved_x = remesh_padded(jnp.pad(section, ((0, 0), (0, 0), (0, 0), (2, 2))), jnp.pad(displace[0], ((0, 0), (0, 0), (2, 2))), 3)
    moved_y = remesh_padded(jnp.pad(moved_x, ((0, 0), (2, 2), (0, 0), (0, 0))), jnp.pad(displace[1], ((2, 2), (0, 0), (0, 0))), 1)
    moved_z = remesh_padded(jnp.pad(moved_y, ((0, 0), (0, 0), (2, 2), (0, 0))), jnp.pad(displace[2], ((0, 0), (2, 2), (0, 0))), 2)
    return (moved_z, sources)
```

```python
import functools

import jax
import jax.numpy as jnp
from jax import lax
from jax.experimental import pallas as pl
from jax.experimental.pallas import tpu as pltpu
from jax.sharding import PartitionSpec as P

TURBINES = 6
BLADES = 3
BP = 64
ROTOR = BLADES * BP
LANES = 128
WINDOW = 256

section_step = 0.4
viscosity = 0.05
tip_speed = 3.0
turn_step = 2.0 * 3.141592653589793 / 720.0
pi = 3.141592653589793

MESH = pl.DeviceIdType.MESH


def remesh_kernel(shift):
    mag = jnp.abs(shift)
    inner = 1.0 - mag * mag * (2.5 - 1.5 * mag)
    outer = 0.5 * (2.0 - mag) * (2.0 - mag) * (1.0 - mag)
    return jnp.where(mag < 1.0, inner, jnp.where(mag < 2.0, outer, 0.0))


def tap_weights(speed):
    d = jnp.clip(section_step * speed, -1.0, 1.0)
    t = jnp.abs(d)
    t2 = t * t
    h = 0.5 * t2 * t
    centre = 1.0 - 2.5 * t2 + 3.0 * h
    toward = 0.5 * t + 2.0 * t2 - 3.0 * h
    away = t2 - 0.5 * t - h
    far = h - 0.5 * t2
    right = d > 0.0
    zero = jnp.zeros_like(d)
    return (
        jnp.where(right, zero, far),
        jnp.where(right, away, toward),
        centre,
        jnp.where(right, toward, away),
        jnp.where(right, far, zero),
    )


def blade_forces(vel, chord, twist, angle, first, count):
    points = first + lax.broadcasted_iota(jnp.int32, (1, count), 1)
    station = points % BP
    blade = points // BP % BLADES
    row = lax.broadcasted_iota(jnp.int32, (8, LANES), 0).astype(jnp.float32)
    theta = angle.astype(jnp.float32) * turn_step + 2.0 * pi / 3.0 * row
    cos_r = jnp.cos(theta)
    sin_r = jnp.sin(theta)
    cos_t = jnp.where(blade == 0, cos_r[0:1, 0:1], jnp.where(blade == 1, cos_r[1:2, 0:1], cos_r[2:3, 0:1]))
    sin_t = jnp.where(blade == 0, sin_r[0:1, 0:1], jnp.where(blade == 1, sin_r[1:2, 0:1], sin_r[2:3, 0:1]))
    radius = (station.astype(jnp.float32) + 0.5) / BP
    rel_x = vel[0]
    rel_y = vel[1] + tip_speed * radius * sin_t
    rel_z = vel[2] - tip_speed * radius * cos_t
    rel_t = -sin_t * rel_y + cos_t * rel_z
    speed = jnp.sqrt(rel_x * rel_x + rel_t * rel_t + 1.0)
    gamma = pi * chord * (rel_x * jnp.cos(twist) + rel_t * jnp.sin(twist))
    before = jnp.where(station == 0, 0.0, pltpu.roll(gamma, 1, 1))
    shed = (gamma - before) / speed
    return (shed * rel_x, gamma * cos_t + shed * rel_y, gamma * sin_t + shed * rel_z)


def split(value):
    high = value.astype(jnp.bfloat16)
    return high, (value - high.astype(jnp.float32)).astype(jnp.bfloat16)


def dot(a, b):
    return jnp.dot(a, b, preferred_element_type=jnp.float32)


def kernel(
    ny, nz, om, ve, cells, fracs, owner, chord, twist, angle, moved, rim, sources,
    F, M, N, smear, d_x, l_x, s_x, slots, acc, tx_h, tx_l, ty, tz, tt_h, tt_l, srow, zsend, zrecv, wsend, wrecv,
    in_sem, out_sem, rim_sem, y_send, y_recv, z_send, z_recv, v_send, v_recv, w_send, w_recv, s_send, s_recv,
):
    cy, cz, nx = om.shape[1], om.shape[2], om.shape[3]
    gy = lax.axis_index("gy")
    gz = lax.axis_index("gz")
    n = ny * nz
    me = gy * nz + gz
    span_blocks = ny // TURBINES
    vert_blocks = max(nz // 2, 1)
    vert_first = (nz - vert_blocks) // 2
    group = span_blocks * vert_blocks
    has = (gy < span_blocks * TURBINES) & (gz >= vert_first) & (gz < vert_first + vert_blocks)
    rotor = lax.min(gy // span_blocks, TURBINES - 1)
    slot = jnp.clip(
        rotor * group + gy % span_blocks * vert_blocks + gz - vert_first, 0, TURBINES * group - 1
    )
    base = pl.multiple_of((rotor // 2) * (2 * ROTOR) + (rotor % 2) * LANES, LANES)
    lo_y, hi_y, lo_z, hi_z = gy > 0, gy < ny - 1, gz > 0, gz < nz - 1
    zin = pl.ds(8, cz)

    load_o = pltpu.make_async_copy(om, F.at[0:3, pl.ds(2, cy), zin], in_sem.at[0])
    load_v = pltpu.make_async_copy(ve, F.at[3:6, pl.ds(2, cy), zin], in_sem.at[1])
    load_v.start()
    load_o.start()

    barrier = pltpu.get_barrier_semaphore()

    def greet(i, carry):
        d = (me + i) % n
        pl.semaphore_signal(barrier, inc=1, device_id={"gy": d // nz, "gz": d % nz}, device_id_type=MESH)
        return carry

    lax.fori_loop(1, n, greet, 0)

    @pl.when(jnp.logical_not(lo_y))
    def _():
        F[:, 0:2, 8 : 8 + cz] = jnp.zeros((6, 2, cz, nx), jnp.float32)
        M[:, 0:2] = jnp.zeros((3, 2, cz, nx), jnp.float32)

    @pl.when(jnp.logical_not(hi_y))
    def _():
        F[:, cy + 2 : cy + 4, 8 : 8 + cz] = jnp.zeros((6, 2, cz, nx), jnp.float32)
        M[:, cy + 2 : cy + 4] = jnp.zeros((3, 2, cz, nx), jnp.float32)

    @pl.when(jnp.logical_not(lo_z))
    def _():
        zrecv[0] = jnp.zeros(zrecv.shape[1:], jnp.float32)
        wrecv[0] = jnp.zeros(wrecv.shape[1:], jnp.float32)

    @pl.when(jnp.logical_not(hi_z))
    def _():
        zrecv[1] = jnp.zeros(zrecv.shape[1:], jnp.float32)
        wrecv[1] = jnp.zeros(wrecv.shape[1:], jnp.float32)

    gap = lax.broadcasted_iota(jnp.int32, (nx, nx), 0) - lax.broadcasted_iota(jnp.int32, (nx, nx), 1)

    def banded(values):
        total = jnp.zeros((nx, nx), jnp.float32)
        for k, value in values.items():
            total = jnp.where(gap == k, value, total)
        return total.astype(jnp.bfloat16)

    first_x = banded({-2: 1.0, -1: -8.0, 1: 8.0, 2: -1.0})
    second_x = banded({-2: -1.0, -1: 16.0, 0: -90.0, 1: 16.0, 2: -1.0})
    for i in range(2):
        d_x[i * nx : (i + 1) * nx] = first_x
        l_x[i * nx : (i + 1) * nx] = second_x
    for i, k in enumerate((-2, -1, 1, 2)):
        move = banded({-k: 1.0})
        s_x[2 * i * nx : (2 * i + 1) * nx] = move
        s_x[(2 * i + 1) * nx : (2 * i + 2) * nx] = move

    pl.semaphore_wait(barrier, n - 1)

    def remote(src, dst, send, recv, to_y, to_z):
        return pltpu.make_async_remote_copy(
            src_ref=src, dst_ref=dst, send_sem=send, recv_sem=recv,
            device_id={"gy": to_y, "gz": to_z}, device_id_type=MESH,
        )

    up_y = lax.min(gy + 1, ny - 1)
    dn_y = lax.max(gy - 1, 0)
    up_z = lax.min(gz + 1, nz - 1)
    dn_z = lax.max(gz - 1, 0)
    y_up = [
        [
            remote(a.at[c, pl.ds(cy - 2, 2)], F.at[3 * i + c, 0:2, zin], y_send.at[6 * i + c], y_recv.at[6 * i + c], up_y, gz)
            for i, a in enumerate((om, ve))
        ]
        for c in range(3)
    ]
    y_dn = [
        [
            remote(a.at[c, pl.ds(0, 2)], F.at[3 * i + c, pl.ds(cy + 2, 2), zin], y_send.at[6 * i + 3 + c], y_recv.at[6 * i + 3 + c], dn_y, gz)
            for i, a in enumerate((om, ve))
        ]
        for c in range(3)
    ]
    for c in range(3):

        @pl.when(hi_y)
        def _(c=c):
            y_up[c][0].start()
            y_up[c][1].start()

        @pl.when(lo_y)
        def _(c=c):
            y_dn[c][0].start()
            y_dn[c][1].start()

    load_v.wait()

    load_o.wait()

    for side, row in ((0, cz - 2), (1, 0)):
        for c in range(6):
            zsend[side, c] = F[c, 2 : 2 + cy, 8 + row : 10 + row, :]
    z_copy = [
        remote(zsend.at[0], zrecv.at[0], z_send.at[0], z_recv.at[0], gy, up_z),
        remote(zsend.at[1], zrecv.at[1], z_send.at[1], z_recv.at[1], gy, dn_z),
    ]

    @pl.when(hi_z)
    def _():
        z_copy[0].start()

    @pl.when(lo_z)
    def _():
        z_copy[1].start()

    @pl.when(has)
    def _():
        win = pl.ds(base, WINDOW)
        cell = cells[:, win]
        frac = fracs[:, win]
        own = owner[win].reshape(1, WINDOW)

        def table(length, at, which):
            rows = lax.broadcasted_iota(jnp.int32, (length, WINDOW), 0)
            gap = rows + (at - cell[which : which + 1])
            return remesh_kernel(gap.astype(jnp.float32) - frac[which : which + 1])

        t_x = table(nx, 0, 0)
        high, low = split(t_x)
        tx_h[...] = high
        tx_l[...] = low
        high, low = split(t_x.T)
        tt_h[...] = high
        tt_l[...] = low
        ty[...] = table(cy, (gy - own // nz) * cy, 1)
        tz[...] = table(cz, (gz - own % nz) * cz, 2)
        acc[...] = jnp.zeros_like(acc)

        def layer(y, carry):
            block = F[3:6, y + 2, 8 : 8 + cz, :].reshape(3 * cz, nx)
            high, low = split(block)
            both = dot(high, tx_h[...]) + (dot(low, tx_h[...]) + dot(high, tx_l[...]))
            both = both.reshape(3, cz, WINDOW) * tz[...][None]
            acc[0:3, :] += jnp.sum(both, axis=1) * ty[pl.ds(y, 1), :]
            return carry

        lax.fori_loop(0, cy, layer, 0)
        slots[slot, 0:3, :] = acc[0:3, 0:LANES]
        slots[slot, 3:6, :] = acc[0:3, LANES:WINDOW]

        def send_peer(b, carry):
            to_y = rotor * span_blocks + b // vert_blocks
            to_z = vert_first + b % vert_blocks
            d = to_y * nz + to_z

            @pl.when(d != me)
            def _():
                remote(slots.at[slot], slots.at[slot], s_send.at[d], s_recv.at[slot], to_y, to_z).start()

            return carry

        lax.fori_loop(0, group, send_peer, 0)

    def send_rest(i, carry):
        d = (me + i) % n
        to_y, to_z = d // nz, d % nz
        peer = (
            (to_y // span_blocks == rotor) & (to_y < span_blocks * TURBINES)
            & (to_z >= vert_first) & (to_z < vert_first + vert_blocks)
        )

        @pl.when(has & jnp.logical_not(peer))
        def _():
            remote(slots.at[slot], slots.at[slot], s_send.at[d], s_recv.at[slot], to_y, to_z).start()

        return carry

    lax.fori_loop(1, n, send_rest, 0)

    def slot_wait(k):
        @pl.when(jnp.logical_not(has & (k == slot)))
        def _():
            remote(slots.at[k], slots.at[k], s_send.at[0], s_recv.at[k], gy, gz).wait_recv()

    @pl.when(has)
    def _():
        def take(b, carry):
            slot_wait(rotor * group + b)
            tile = slots[rotor * group + b]
            acc[0:3, 0:LANES] += tile[0:3]
            acc[0:3, LANES:WINDOW] += tile[3:6]
            return carry

        acc[...] = jnp.zeros_like(acc)
        lax.fori_loop(0, group, take, 0)
        win = pl.ds(base, WINDOW)
        vel = [acc[c : c + 1, :] for c in range(3)]
        forces = blade_forces(vel, chord[win].reshape(1, WINDOW), twist[win].reshape(1, WINDOW), angle[0], base, WINDOW)
        for c in range(3):
            srow[c : c + 1, :] = section_step * forces[c]

        def layer(y, carry):
            spread = jnp.concatenate([tz[...] * (ty[pl.ds(y, 1), :] * srow[c : c + 1, :]) for c in range(3)], axis=0)
            high, low = split(spread)
            total = dot(high, tt_h[...]) + (dot(low, tt_h[...]) + dot(high, tt_l[...]))
            smear[:, y] = total.reshape(3, cz, nx)
            return carry

        lax.fori_loop(0, cy, layer, 0)

    @pl.when(jnp.logical_not(has))
    def _():
        smear[...] = jnp.zeros_like(smear)

    @pl.when(lo_z)
    def _():
        z_copy[0].wait_recv()

    @pl.when(hi_z)
    def _():
        z_copy[1].wait_recv()

    for c in range(6):
        F[c, 2 : 2 + cy, 6:8, :] = zrecv[0, c]
        F[c, 2 : 2 + cy, 8 + cz : 10 + cz, :] = zrecv[1, c]

    ROWS = 8
    d1 = 1.0 / 12.0

    def section_layer(y, comps=(0, 1, 2)):
        def stencil(start, matrix):
            block = jnp.concatenate([F[start + c, y + 2, 8 : 8 + cz, :] for c in comps], axis=0)
            return dot(jnp.concatenate(split(block), axis=1), matrix[...])

        along = stencil(3, d_x)
        bent = stencil(0, l_x)
        taps = tap_weights(F[3, y + 2, 8 : 8 + cz, :])
        w = [F[c, y + 2, 8 : 8 + cz, :] for c in range(3)]
        kept, sides = [], []
        for i, c in enumerate(comps):
            def yv(a, k):
                return F[a, y + 2 + k, 8 : 8 + cz, :]

            def zv(a, k):
                return F[a, y + 2, 8 + k : 8 + k + cz, :]

            v = 3 + c
            rows = slice(i * cz, (i + 1) * cz)
            dy = 8.0 * (yv(v, 1) - yv(v, -1)) - (yv(v, 2) - yv(v, -2))
            dz = 8.0 * (zv(v, 1) - zv(v, -1)) - (zv(v, 2) - zv(v, -2))
            stretch = w[2] * along[rows] + w[1] * dz + w[0] * dy
            near = (yv(c, 1) + yv(c, -1)) + (zv(c, 1) + zv(c, -1))
            wide = (yv(c, 2) + yv(c, -2)) + (zv(c, 2) + zv(c, -2))
            lap = 16.0 * near - wide + bent[rows]
            value = w[c] + (section_step * d1) * (stretch + viscosity * lap) + smear[c, y]
            kept.append(taps[2] * value)
            pieces = []
            for k in (0, 1, 3, 4):
                pieces.extend(split(taps[k] * value))
            sides.append(jnp.concatenate(pieces, axis=1))
        total = dot(jnp.concatenate(sides, axis=0), s_x[...])
        for i, c in enumerate(comps):
            M[c, y + 2] = kept[i] + total[i * cz : (i + 1) * cz]

    def span_layer(y, comps=(0, 1, 2)):
        for z0 in range(0, cz, ROWS):
            totals = {}
            for k in range(-2, 3):
                weight = tap_weights(F[4, y + 2 - k, 8 + z0 : 8 + z0 + ROWS, :])[k + 2]
                for c in comps:
                    part = weight * M[c, y + 2 - k, z0 : z0 + ROWS, :]
                    totals[c] = totals[c] + part if c in totals else part
            for c in comps:
                N[c, y, z0 : z0 + ROWS, :] = totals[c]

    def over(first, last, body):
        def step(y, carry):
            body(y)
            return carry

        lax.fori_loop(first, last, step, 0)

    def over_edges(body):
        def step(i, carry):
            body(jnp.where(i < 2, i, cy - 4 + i))
            return carry

        lax.fori_loop(0, 4, step, 0)

    over(2, cy - 2, section_layer)

    v_up, v_dn = [], []
    for c in range(3):

        @pl.when(lo_y)
        def _(c=c):
            y_up[c][0].wait_recv()
            y_up[c][1].wait_recv()

        @pl.when(hi_y)
        def _(c=c):
            y_dn[c][0].wait_recv()
            y_dn[c][1].wait_recv()

        over_edges(functools.partial(section_layer, comps=(c,)))
        v_up.append(remote(M.at[c, pl.ds(cy, 2)], M.at[c, 0:2], v_send.at[c], v_recv.at[c], up_y, gz))
        v_dn.append(remote(M.at[c, 2:4], M.at[c, pl.ds(cy + 2, 2)], v_send.at[3 + c], v_recv.at[3 + c], dn_y, gz))

        @pl.when(hi_y)
        def _(c=c):
            v_up[c].start()

        @pl.when(lo_y)
        def _(c=c):
            v_dn[c].start()

    over(2, cy - 2, span_layer)
    stores = [
        pltpu.make_async_copy(N.at[:, part], moved.at[:, part], out_sem.at[i])
        for i, part in enumerate((pl.ds(2, cy - 4), pl.ds(0, 2), pl.ds(cy - 2, 2)))
    ]
    stores[0].start()
    w_copy = [[], []]

    def rims(number, first, length):
        for side, row in ((0, cz - 2), (1, 0)):
            for c in range(3):
                wsend[side, c, first : first + length] = N[c, first : first + length, row : row + 2, :]
            w_copy[side].append(remote(
                wsend.at[side, :, first : first + length], wrecv.at[side, 0:3, first : first + length],
                w_send.at[2 * number + side], w_recv.at[2 * number + side], gy, (up_z, dn_z)[side],
            ))

        @pl.when(hi_z)
        def _():
            w_copy[0][number].start()

        @pl.when(lo_z)
        def _():
            w_copy[1][number].start()

    rims(0, 2, cy - 4)

    count = sources.shape[1]
    sources[...] = jnp.zeros_like(sources)

    for t in range(TURBINES):
        first = (t // 2) * (2 * ROTOR) + (t % 2) * LANES

        def gather(b, carry, t=t, first=first):
            k = t * group + b

            @pl.when(jnp.logical_not(has & (rotor == t)))
            def _():
                slot_wait(k)

            tile = slots[k]
            sources[0:3, first : first + LANES] += tile[0:3]
            sources[0:3, first + LANES : first + WINDOW] += tile[3:6]
            return carry

        lax.fori_loop(0, group, gather, 0)
    forces = blade_forces(
        [sources[c : c + 1, :] for c in range(3)], chord[...].reshape(1, count), twist[...].reshape(1, count),
        angle[0], 0, count,
    )
    for c in range(3):
        sources[c : c + 1, :] = forces[c]

    for c in range(3):

        @pl.when(lo_y)
        def _(c=c):
            v_up[c].wait_recv()

        @pl.when(hi_y)
        def _(c=c):
            v_dn[c].wait_recv()

        over_edges(functools.partial(span_layer, comps=(c,)))

    stores[1].start()
    stores[2].start()
    rims(1, 0, 2)
    rims(2, cy - 2, 2)
    for side in range(2):
        wrecv[side, 3] = zrecv[side, 5]
    for i in range(3):

        @pl.when(lo_z)
        def _(i=i):
            w_copy[0][i].wait_recv()

        @pl.when(hi_z)
        def _(i=i):
            w_copy[1][i].wait_recv()

    rim_store = pltpu.make_async_copy(wrecv, rim, rim_sem)
    rim_store.start()

    @pl.when(hi_y)
    def _():
        for c in range(3):
            y_up[c][0].wait_send()
            y_up[c][1].wait_send()
            v_up[c].wait_send()

    @pl.when(lo_y)
    def _():
        for c in range(3):
            y_dn[c][0].wait_send()
            y_dn[c][1].wait_send()
            v_dn[c].wait_send()

    @pl.when(hi_z)
    def _():
        z_copy[0].wait_send()
        for i in range(3):
            w_copy[0][i].wait_send()

    @pl.when(lo_z)
    def _():
        z_copy[1].wait_send()
        for i in range(3):
            w_copy[1][i].wait_send()

    def sent(i, carry):
        d = (me + i) % n

        @pl.when(has)
        def _():
            remote(slots.at[slot], slots.at[slot], s_send.at[d], s_recv.at[0], gy, gz).wait_send()

        return carry

    lax.fori_loop(1, n, sent, 0)
    for store in stores:
        store.wait()
    rim_store.wait()


def vertical_kernel(moved, speed, rim, given, out, sources, G):
    _, rows, cz, nx = moved.shape
    for c in range(4):
        G[c, :, 8 : 8 + cz, :] = moved[c] if c < 3 else speed[0]
        G[c, :, 6:8, :] = rim[0, c]
        G[c, :, 8 + cz : 10 + cz, :] = rim[1, c]
    sources[...] = given[...]

    def layer(y, carry):
        for z0 in range(0, cz, 8):
            totals = [None] * 3
            for k in range(-2, 3):
                at = 8 + z0 - k
                weight = tap_weights(G[3, y, at : at + 8, :])[k + 2]
                for c in range(3):
                    part = weight * G[c, y, at : at + 8, :]
                    totals[c] = part if totals[c] is None else totals[c] + part
            for c in range(3):
                out[c, y, z0 : z0 + 8, :] = totals[c]
        return carry

    lax.fori_loop(0, rows, layer, 0)


def on_device(ny, nz, omega, velocity, point_owner, point_cells, point_frac, chord, twist, angle_step):
    _, cy, cz, nx = omega.shape
    points = point_owner.shape[0]
    n = ny * nz
    nslots = TURBINES * (ny // TURBINES) * max(nz // 2, 1)
    f32, bf16 = jnp.float32, jnp.bfloat16
    vmem = pl.BlockSpec(memory_space=pltpu.VMEM)
    hbm = pl.BlockSpec(memory_space=pl.ANY)
    given = pl.BlockSpec(memory_space=pltpu.HBM)
    dma = pltpu.SemaphoreType.DMA
    moved, rim, sources = pl.pallas_call(
        functools.partial(kernel, ny, nz),
        out_shape=(
            jax.ShapeDtypeStruct(omega.shape, f32),
            jax.ShapeDtypeStruct((2, 4, cy, 2, nx), f32),
            jax.ShapeDtypeStruct((3, points), f32),
        ),
        in_specs=[given, given, vmem, vmem, vmem, vmem, vmem, pl.BlockSpec(memory_space=pltpu.SMEM)],
        out_specs=(hbm, hbm, vmem),
        scratch_shapes=[
            pltpu.VMEM((6, cy + 4, cz + 16, nx), f32),
            pltpu.VMEM((3, cy + 4, cz, nx), f32),
            pltpu.VMEM((3, cy, cz, nx), f32),
            pltpu.VMEM((3, cy, cz, nx), f32),
            pltpu.VMEM((2 * nx, nx), bf16),
            pltpu.VMEM((2 * nx, nx), bf16),
            pltpu.VMEM((8 * nx, nx), bf16),
            pltpu.VMEM((nslots, 8, LANES), f32),
            pltpu.VMEM((8, WINDOW), f32),
            pltpu.VMEM((nx, WINDOW), bf16),
            pltpu.VMEM((nx, WINDOW), bf16),
            pltpu.VMEM((cy, WINDOW), f32),
            pltpu.VMEM((cz, WINDOW), f32),
            pltpu.VMEM((WINDOW, nx), bf16),
            pltpu.VMEM((WINDOW, nx), bf16),
            pltpu.VMEM((8, WINDOW), f32),
            pltpu.VMEM((2, 6, cy, 2, nx), f32),
            pltpu.VMEM((2, 6, cy, 2, nx), f32),
            pltpu.VMEM((2, 3, cy, 2, nx), f32),
            pltpu.VMEM((2, 4, cy, 2, nx), f32),
            dma((2,)),
            dma((3,)),
            dma,
            dma((12,)),
            dma((12,)),
            dma((2,)),
            dma((2,)),
            dma((6,)),
            dma((6,)),
            dma((6,)),
            dma((6,)),
            dma((n,)),
            dma((nslots,)),
        ],
        compiler_params=pltpu.CompilerParams(
            collective_id=0, has_side_effects=True, vmem_limit_bytes=60 * 1024 * 1024
        ),
        name="wake_step",
    )(
        omega,
        velocity,
        point_cells,
        point_frac,
        point_owner,
        chord,
        twist,
        angle_step,
    )
    rows = 4 if cy % 4 == 0 else cy
    every = pl.BlockSpec((3, points), lambda i: (0, 0))
    field = pl.BlockSpec((3, rows, cz, nx), lambda i: (0, i, 0, 0))
    return pl.pallas_call(
        vertical_kernel,
        out_shape=(
            jax.ShapeDtypeStruct(omega.shape, f32),
            jax.ShapeDtypeStruct((3, points), f32),
        ),
        grid=(cy // rows,),
        in_specs=[
            field,
            pl.BlockSpec((1, rows, cz, nx), lambda i: (2, i, 0, 0)),
            pl.BlockSpec((2, 4, rows, 2, nx), lambda i: (0, 0, i, 0, 0)),
            every,
        ],
        out_specs=(field, every),
        scratch_shapes=[pltpu.VMEM((4, rows, cz + 16, nx), f32)],
        compiler_params=pltpu.CompilerParams(vmem_limit_bytes=16 * 1024 * 1024),
        name="wake_vertical",
    )(moved, velocity, rim, sources)


def solution(mesh):
    in_specs = (P(None, "gy", "gz", None), P(None, "gy", "gz", None), P(), P(), P(), P(), P(), P())
    out_specs = (P(None, "gy", "gz", None), P())
    return jax.shard_map(
        functools.partial(on_device, mesh.shape["gy"], mesh.shape["gz"]),
        mesh=mesh, in_specs=in_specs, out_specs=out_specs, check_vma=False,
    )
```
